32 devices in a mesh: sensor: 8 (over y, x, core), batch: 4 (over z).
Axes of the slice: x: 2, y: 2, z: 4, core: 2. Of those that a mesh axis runs over, the one named last changes fastest.
Arguments:
- samples: bfloat16 [512, 16384], P('batch', 'sensor'), may hold values from -6 to 6
- branch_weight: bfloat16 [16384, 2048], P('sensor', 'batch'), may hold values from -0.046875 to 0.046875
- branch_bias: float32 [2048], P('batch'), may hold values from -3 to 3
- upstream: bfloat16 [512, 2048], P('sensor', 'batch'), may hold values from -0.29882812 to 0.29882812
Outputs:
- activation: bfloat16 [512, 2048], P('sensor', 'batch')
- weight_grad: bfloat16 [16384, 2048], P('sensor', 'batch')
- bias_grad: float32 [2048], P('batch')
The draws below stay inside these ranges and needn't reach their ends.
All inputs are finite; a program needn't handle non-finite values.
Results may differ from the reference program's by a relative error of at most 0.005.
Values may be sent and summed in bfloat16 or wider, within the bound.
No kernel may reach another device: no remote copies, remote signals or barrier semaphores. Data moves between devices by JAX's collectives and lax.ppermute only.
A program may use at most 64 MiB of HBM per device.

```python
import jax
import jax.numpy as jnp
from jax import lax

HIDDEN_SIZE = 2048
SENSORS = 16384
FUNCS = 512


def spiked(result, stream_key, source, target, parts, factor):
    owner, partner = [(jnp.arange(result.shape[axis_at]) // (result.shape[axis_at] // parts)).reshape([-1 if axis == axis_at else 1 for axis in range(result.ndim)]) for axis_at in (source, target)]
    chosen = jax.random.permutation(stream_key, parts)[partner]
    strong = (owner == chosen) | (owner == (partner + parts // 2) % parts)
    return jnp.where(strong, factor * result, result)


def block_scale(own_key, shape, split, low, top_value):
    gain = 1.0
    for axis_at, parts in split:
        steps = jax.random.uniform(jax.random.fold_in(jax.random.fold_in(own_key, 6), axis_at), (parts,), jnp.float32, low / len(split), top_value / len(split))
        gain = gain * jnp.repeat(jnp.exp(steps), shape[axis_at] // parts).reshape((-1,) + (1,) * (len(shape) - 1 - axis_at))
    return gain


def centred(own_key, shape, deviation, limit, split=(), kind=jnp.bfloat16):
    result = deviation * jax.random.normal(own_key, shape, jnp.float32)
    if split:
        result = result * block_scale(own_key, shape, split, -0.22, 0.18)
    return jnp.clip(result, -limit, limit).astype(kind)


def heavy_noise(stream_key, shape, spread, limit, pieces, heavy, held_as=jnp.bfloat16):
    result = spread * jax.random.normal(stream_key, shape, jnp.float32)
    if pieces:
        result = result * block_scale(stream_key, shape, pieces, -0.22, 0.18)
    return jnp.clip(spiked(result, jax.random.fold_in(stream_key, 3), *heavy), -limit, limit).astype(held_as)


def setup_inputs(seed: int = 0) -> dict:
    seeds = jax.random.split(jax.random.key(seed), 5)
    samples = heavy_noise(seeds[0], (FUNCS, SENSORS), 1.0, 6.0, ((0, 4), (1, 8)), (1, 0, 8, 2.0))
    branch_weight = centred(seeds[1], (SENSORS, HIDDEN_SIZE), SENSORS ** -0.5, 0.046875, ((0, 8), (1, 4)))
    branch_bias = centred(seeds[2], (HIDDEN_SIZE,), 0.5, 3.0, ((0, 4),), jnp.float32)
    upstream = centred(seeds[3], (FUNCS, HIDDEN_SIZE), 0.05, 0.29882812, ((0, 8), (1, 4)))
    return dict(samples=samples, branch_weight=branch_weight, branch_bias=branch_bias, upstream=upstream)


def reference(samples, branch_weight, branch_bias, upstream):
    pre = jnp.dot(samples, branch_weight, preferred_element_type=jnp.float32) + branch_bias.astype(jnp.float32)[None, :]
    act_full = jnp.tanh(pre)
    activation = act_full.astype(jnp.bfloat16)
    grad_pre = (upstream.astype(jnp.float32) * (1.0 - act_full * act_full)).astype(jnp.bfloat16)
    weight_grad = lax.dot_general(samples, grad_pre, (((0,), (0,)), ((), ())), preferred_element_type=jnp.float32).astype(jnp.bfloat16)
    bias_grad = jnp.sum(grad_pre.astype(jnp.float32), axis=0)
    return activation, weight_grad, bias_grad
```

```python
import functools

import jax
import jax.numpy as jnp
from jax import lax
from jax.experimental import pallas as pl
from jax.experimental.pallas import tpu as pltpu
from jax.sharding import PartitionSpec as P


HALVES = 2
VMEM = pl.BlockSpec(memory_space=pltpu.VMEM)


def plain(samples, branch_weight, branch_bias, upstream):
    all_rows = lax.all_gather(samples, "batch", axis=0, tiled=True)
    partial_value = jnp.dot(all_rows, branch_weight, preferred_element_type=jnp.float32)
    summed = lax.psum_scatter(partial_value, "sensor", scatter_dimension=0, tiled=True)
    pre = summed + branch_bias[None, :]
    act_full = jnp.tanh(pre)
    activation = act_full.astype(jnp.bfloat16)
    grad_pre = (upstream.astype(jnp.float32) * (1.0 - act_full * act_full)).astype(jnp.bfloat16)
    grad_all = lax.all_gather(grad_pre, "sensor", axis=0, tiled=True)
    weight_full = lax.dot_general(
        all_rows, grad_all, (((0,), (0,)), ((), ())), preferred_element_type=jnp.float32
    )
    row_total = jnp.sum(grad_all.astype(jnp.float32), axis=0)
    return activation, weight_full.astype(jnp.bfloat16), row_total


def transpose_kernel(*refs):
    ins, out = refs[:-1], refs[-1]
    at = 0
    for ref in ins:
        width = ref.shape[1]
        out[at : at + width, :] = ref[...].T
        at += width


def transposed(parts):
    rows = parts[0].shape[0]
    width = sum(p.shape[1] for p in parts)
    nbytes = rows * width * 2
    return pl.pallas_call(
        transpose_kernel,
        out_shape=jax.ShapeDtypeStruct((width, rows), parts[0].dtype),
        in_specs=[VMEM] * len(parts),
        out_specs=VMEM,
        compiler_params=pltpu.CompilerParams(vmem_limit_bytes=8 << 20),
        cost_estimate=pl.CostEstimate(flops=nbytes * 64, bytes_accessed=2 * nbytes, transcendentals=0),
    )(*parts)


def load_kernel(start, source, out, sem):
    copy = pltpu.make_async_copy(source.at[:, start : start + out.shape[1]], out, sem)
    copy.start()
    copy.wait()


def loaded(samples, start, width):
    rows = samples.shape[0]
    return pl.pallas_call(
        functools.partial(load_kernel, start),
        out_shape=jax.ShapeDtypeStruct((rows, width), samples.dtype),
        in_specs=[pl.BlockSpec(memory_space=pltpu.HBM)],
        out_specs=VMEM,
        scratch_shapes=[pltpu.SemaphoreType.DMA],
        compiler_params=pltpu.CompilerParams(vmem_limit_bytes=4 << 20),
        cost_estimate=pl.CostEstimate(flops=1 << 20, bytes_accessed=4 * rows * width, transcendentals=0),
    )(samples)


def finish_kernel(counts, slots, tile, at, *refs):
    n = len(counts)
    lefts, refs = refs[:slots], refs[slots:]
    mine, theirs, acts, refs = refs[:n], refs[n : 2 * n], refs[2 * n : 3 * n], refs[3 * n :]
    out, act_out, total_out, grad, staged, act_staged, total, sems = refs
    core, chosen = at[0], at[1]
    half = mine[0].shape[1]
    slot = 0
    for count, own, other, act in zip(counts, mine, theirs, acts):
        for i in range(count):
            base = slot * 2 * half
            grad[pl.ds(pl.multiple_of(base + core * half, half), half), :] = own[i]
            grad[pl.ds(pl.multiple_of(base + (1 - core) * half, half), half), :] = other[i]

            @pl.when(chosen == slot)
            def _(act=act, i=i):
                act_staged[...] = act[i]

            slot += 1
    sends = [pltpu.make_async_copy(act_staged, act_out, sems.at[0])]
    sends[0].start()
    width = lefts[0].shape[0]
    for k in range(width // tile):
        rows = slice(k * tile, (k + 1) * tile)
        left = jnp.concatenate([ref[rows, :] for ref in lefts], axis=1)
        staged[rows, :] = jnp.dot(left, grad[...], preferred_element_type=jnp.float32).astype(staged.dtype)
        send = pltpu.make_async_copy(staged.at[rows, :], out.at[rows, :], sems.at[2 + k])
        send.start()
        sends.append(send)
    total[...] = jnp.sum(grad[...].astype(jnp.float32), axis=0, keepdims=True)
    send = pltpu.make_async_copy(total, total_out, sems.at[1])
    send.start()
    sends.append(send)
    for send in sends:
        send.wait()


def finish(lefts, mine, theirs, acts, at):
    width, _ = lefts[0].shape
    counts = tuple(g.shape[0] for g in mine)
    _, half, columns = mine[0].shape
    rows = 2 * half * len(lefts)
    tile = 256
    hbm = pl.BlockSpec(memory_space=pl.ANY)
    kind = mine[0].dtype
    out, act, total = pl.pallas_call(
        functools.partial(finish_kernel, counts, len(lefts), tile),
        out_shape=(
            jax.ShapeDtypeStruct((width, columns), kind),
            jax.ShapeDtypeStruct((half, columns), kind),
            jax.ShapeDtypeStruct((1, columns), jnp.float32),
        ),
        in_specs=[pl.BlockSpec(memory_space=pltpu.SMEM)] + [VMEM] * (len(lefts) + 3 * len(counts)),
        out_specs=(hbm, hbm, hbm),
        scratch_shapes=[
            pltpu.VMEM((rows, columns), kind),
            pltpu.VMEM((width, columns), kind),
            pltpu.VMEM((half, columns), kind),
            pltpu.VMEM((1, columns), jnp.float32),
            pltpu.SemaphoreType.DMA((2 + width // tile,)),
        ],
        compiler_params=pltpu.CompilerParams(vmem_limit_bytes=24 << 20),
        cost_estimate=pl.CostEstimate(
            flops=2 * width * columns * rows, bytes_accessed=4 * width * columns, transcendentals=0
        ),
    )(at, *lefts, *mine, *theirs, *acts)
    return act, out, total.reshape(columns)


def pipelined(chips, samples, weight, bias, upstream):
    _, width = samples.shape
    columns = weight.shape[1]
    half = upstream.shape[0]
    z = lax.axis_index("batch")
    s = lax.axis_index("sensor")
    core, chip = s & 1, s >> 1
    is_end = (z == 0) | (z == 3)
    blocks = [z, z ^ 1, z ^ jnp.where(is_end, 2, 3), z ^ jnp.where(is_end, 3, 2)]
    from_chip = [b ^ chip for b in blocks]
    chosen = sum(jnp.where(f == 0, j, 0) for j, f in enumerate(from_chip))
    at = jnp.stack([core, chosen]).astype(jnp.int32)
    samples, weight, core, other, is_end, from_chip, at = lax.optimization_barrier(
        (samples, weight, core, 1 - core, is_end, from_chip, at)
    )

    def along(value, pairs):
        return lax.ppermute(value, "batch", pairs)

    def across(value, masks):
        return lax.ppermute(value, "sensor", [(i, i ^ masks[i % 2]) for i in range(2 * chips)])

    outer = [(0, 1), (1, 0), (2, 3), (3, 2)]
    inner = [(1, 2), (2, 1)]
    outward = [(1, 0), (2, 3)]
    step = width // HALVES
    own = []
    for h in range(HALVES):
        own.append(loaded(samples, h * step, step))
    held = loaded(weight, 0, columns)
    first = [along(v, outer) for v in own]
    middle = [along(v, inner) for v in own]
    far = [along(v, inner) for v in first]
    middle_out = [along(v, outward) for v in middle]
    far_out = [along(v, outward) for v in far]
    slots = [
        own,
        first,
        [jnp.where(is_end, a, b) for a, b in zip(middle_out, middle)],
        [jnp.where(is_end, a, b) for a, b in zip(far_out, far)],
    ]
    lefts = []
    for parts in slots:
        lefts.append(transposed(parts))

    def picked(array, index, axis=0):
        size = [1 if d == axis else n for d, n in enumerate(array.shape)]
        start = [index if d == axis else 0 for d in range(array.ndim)]
        return lax.dynamic_slice(array, start, size, allow_negative_indices=False).squeeze(axis)

    ups = jnp.stack([upstream] + [across(upstream, (2 * m, 2 * m)) for m in range(1, chips)])

    def product(j):
        total = None
        for h, part in enumerate(slots[j]):
            term = jnp.dot(part, held[h * step : (h + 1) * step], preferred_element_type=jnp.float32)
            total = lax.optimization_barrier(term) if total is None else total + term
        return total

    def chip_sum(members):
        value = jnp.stack([product(j) for j in members]).reshape(len(members), 2, half, columns)
        return picked(value, core, 1) + across(picked(value, other, 1), (1, 1))

    def outcome(total, members):
        total, shift = lax.optimization_barrier((total, bias))
        act = jnp.tanh(total + shift)
        up = jnp.stack([picked(ups, from_chip[j]) for j in members]).astype(jnp.float32)
        grad = (up * (1.0 - act * act)).astype(jnp.bfloat16)
        return grad, across(grad, (1, 1)), act.astype(jnp.bfloat16)

    x_then_y, y_then_x = (2, 4), (4, 2)
    early = chip_sum([0, 1])
    early = early + across(early, x_then_y)
    both = jnp.concatenate([early, chip_sum([2])])
    both = both + across(both, y_then_x)
    early, third = both[:2], both[2:]
    third = third + across(third, x_then_y)
    last = chip_sum([3])
    last = last + across(last, x_then_y)
    last = last + across(last, y_then_x)
    mine, theirs, acts = zip(*[outcome(early, [0, 1]), outcome(third, [2]), outcome(last, [3])])
    return finish(lefts, mine, theirs, acts, at)


def solution(mesh):
    placed = (P("batch", "sensor"), P("sensor", "batch"), P("batch"), P("sensor", "batch"))
    sensors, batch = mesh.shape["sensor"], mesh.shape["batch"]

    def body(samples, weight, bias, upstream):
        return pipelined(sensors // 2, samples, weight, bias, upstream)

    fits = batch == 4 and sensors == 2 * batch
    return jax.shard_map(
        body if fits else plain,
        mesh=mesh,
        in_specs=placed,
        out_specs=(P("sensor", "batch"), P("sensor", "batch"), P("batch")),
        check_vma=False,
    )
```

```python
import functools

import jax
import jax.numpy as jnp
from jax import lax
from jax.experimental import pallas as pl
from jax.experimental.pallas import tpu as pltpu
from jax.sharding import PartitionSpec as P


HALVES = 2
TILES = 8
VMEM = pl.BlockSpec(memory_space=pltpu.VMEM)


def plain(samples, branch_weight, branch_bias, upstream):
    all_rows = lax.all_gather(samples, "batch", axis=0, tiled=True)
    partial_value = jnp.dot(all_rows, branch_weight, preferred_element_type=jnp.float32)
    summed = lax.psum_scatter(partial_value, "sensor", scatter_dimension=0, tiled=True)
    pre = summed + branch_bias[None, :]
    act_full = jnp.tanh(pre)
    activation = act_full.astype(jnp.bfloat16)
    grad_pre = (upstream.astype(jnp.float32) * (1.0 - act_full * act_full)).astype(jnp.bfloat16)
    grad_all = lax.all_gather(grad_pre, "sensor", axis=0, tiled=True)
    weight_full = lax.dot_general(
        all_rows, grad_all, (((0,), (0,)), ((), ())), preferred_element_type=jnp.float32
    )
    row_total = jnp.sum(grad_all.astype(jnp.float32), axis=0)
    return activation, weight_full.astype(jnp.bfloat16), row_total


def transpose_kernel(*refs):
    ins, out = refs[:-1], refs[-1]
    at = 0
    for ref in ins:
        width = ref.shape[1]
        out[at : at + width, :] = ref[...].T
        at += width


def transposed(parts):
    rows = parts[0].shape[0]
    width = sum(p.shape[1] for p in parts)
    nbytes = rows * width * 2
    return pl.pallas_call(
        transpose_kernel,
        out_shape=jax.ShapeDtypeStruct((width, rows), parts[0].dtype),
        in_specs=[VMEM] * len(parts),
        out_specs=VMEM,
        compiler_params=pltpu.CompilerParams(vmem_limit_bytes=8 << 20),
        cost_estimate=pl.CostEstimate(flops=nbytes * 64, bytes_accessed=2 * nbytes, transcendentals=0),
    )(*parts)


def load_kernel(start, source, out, sem):
    copy = pltpu.make_async_copy(source.at[:, start : start + out.shape[1]], out, sem)
    copy.start()
    copy.wait()


def loaded(samples, start, width):
    rows = samples.shape[0]
    return pl.pallas_call(
        functools.partial(load_kernel, start),
        out_shape=jax.ShapeDtypeStruct((rows, width), samples.dtype),
        in_specs=[pl.BlockSpec(memory_space=pltpu.HBM)],
        out_specs=VMEM,
        scratch_shapes=[pltpu.SemaphoreType.DMA],
        compiler_params=pltpu.CompilerParams(vmem_limit_bytes=4 << 20),
        cost_estimate=pl.CostEstimate(flops=1 << 20, bytes_accessed=4 * rows * width, transcendentals=0),
    )(samples)


def places():
    z, s = lax.axis_index("batch"), lax.axis_index("sensor")
    core, chip = s & 1, s >> 1
    is_end = (z == 0) | (z == 3)
    blocks = [z, z ^ 1, z ^ jnp.where(is_end, 2, 3), z ^ jnp.where(is_end, 3, 2)]
    return core, is_end, [b ^ chip for b in blocks]


def outcome_kernel(members, own, got, bias, ups, grad, act):
    _, _, owners = places()
    for i, member in enumerate(members):
        value = jnp.tanh(own[i] + got[i] + bias[...])
        act[i] = value.astype(act.dtype)
        grad[i] = (ups[owners[member]].astype(jnp.float32) * (1.0 - value * value)).astype(grad.dtype)


def outcome(members, own, got, bias, ups):
    shape = jax.ShapeDtypeStruct(own.shape, ups.dtype)
    return pl.pallas_call(
        functools.partial(outcome_kernel, members),
        out_shape=(shape, shape),
        in_specs=[VMEM] * 4,
        out_specs=(VMEM, VMEM),
        compiler_params=pltpu.CompilerParams(vmem_limit_bytes=4 << 20),
        cost_estimate=pl.CostEstimate(flops=own.size * 8, bytes_accessed=own.size * 12, transcendentals=own.size),
    )(own, got, bias, ups)


def gather_rows(grad, core, mine, theirs):
    slot = 0
    for own, other in zip(mine, theirs):
        count, half, _ = own.shape
        for i in range(count):
            base = slot * 2 * half
            grad[pl.ds(pl.multiple_of(base + core * half, half), half), :] = own[i]
            grad[pl.ds(pl.multiple_of(base + (1 - core) * half, half), half), :] = other[i]
            slot += 1


def tiles(width):
    tile = width // TILES
    return [slice(k * tile, (k + 1) * tile) for k in range(TILES)]


def early_kernel(slots, rounds, *refs):
    lefts, refs = refs[:slots], refs[slots:]
    mine, theirs, refs = refs[:rounds], refs[rounds : 2 * rounds], refs[2 * rounds :]
    acc, total, grad = refs
    gather_rows(grad, places()[0], mine, theirs)
    for rows in tiles(acc.shape[0]):
        left = jnp.concatenate([ref[rows, :] for ref in lefts], axis=1)
        acc[rows, :] = jnp.dot(left, grad[...], preferred_element_type=jnp.float32)
    total[...] = jnp.sum(grad[...].astype(jnp.float32), axis=0, keepdims=True)


def finish_kernel(counts, acc, before, left, own, other, *refs):
    acts, refs = refs[: len(counts)], refs[len(counts) :]
    out, act_out, total_out, grad, staged, act_staged, total, sems = refs
    core, _, owners = places()
    slot = 0
    for count, act in zip(counts, acts):
        for i in range(count):

            @pl.when(owners[slot] == 0)
            def _(act=act, i=i):
                act_staged[...] = act[i]

            slot += 1
    sends = [pltpu.make_async_copy(act_staged, act_out, sems.at[0])]
    sends[0].start()
    gather_rows(grad, core, [own], [other])
    for k, rows in enumerate(tiles(acc.shape[0])):
        term = jnp.dot(left[rows, :], grad[...], preferred_element_type=jnp.float32)
        staged[rows, :] = (acc[rows, :] + term).astype(staged.dtype)
        send = pltpu.make_async_copy(staged.at[rows, :], out.at[rows, :], sems.at[2 + k])
        send.start()
        sends.append(send)
    total[...] = before[...] + jnp.sum(grad[...].astype(jnp.float32), axis=0, keepdims=True)
    send = pltpu.make_async_copy(total, total_out, sems.at[1])
    send.start()
    sends.append(send)
    for send in sends:
        send.wait()


def early_gradient(lefts, mine, theirs):
    width, rows = lefts[0].shape
    columns = mine[0].shape[2]
    depth = rows * len(lefts)
    return pl.pallas_call(
        functools.partial(early_kernel, len(lefts), len(mine)),
        out_shape=(
            jax.ShapeDtypeStruct((width, columns), jnp.float32),
            jax.ShapeDtypeStruct((1, columns), jnp.float32),
        ),
        in_specs=[VMEM] * (len(lefts) + 2 * len(mine)),
        out_specs=(VMEM, VMEM),
        scratch_shapes=[pltpu.VMEM((depth, columns), mine[0].dtype)],
        compiler_params=pltpu.CompilerParams(vmem_limit_bytes=16 << 20),
        cost_estimate=pl.CostEstimate(
            flops=2 * width * columns * depth, bytes_accessed=4 * width * columns, transcendentals=0
        ),
    )(*lefts, *mine, *theirs)


def finish(acc, before, left, own, other, acts):
    width, rows = left.shape
    counts = tuple(a.shape[0] for a in acts)
    _, half, columns = own.shape
    hbm = pl.BlockSpec(memory_space=pl.ANY)
    kind = own.dtype
    out, act, total = pl.pallas_call(
        functools.partial(finish_kernel, counts),
        out_shape=(
            jax.ShapeDtypeStruct((width, columns), kind),
            jax.ShapeDtypeStruct((half, columns), kind),
            jax.ShapeDtypeStruct((1, columns), jnp.float32),
        ),
        in_specs=[VMEM] * (5 + len(acts)),
        out_specs=(hbm, hbm, hbm),
        scratch_shapes=[
            pltpu.VMEM((rows, columns), kind),
            pltpu.VMEM((width, columns), kind),
            pltpu.VMEM((half, columns), kind),
            pltpu.VMEM((1, columns), jnp.float32),
            pltpu.SemaphoreType.DMA((2 + TILES,)),
        ],
        compiler_params=pltpu.CompilerParams(vmem_limit_bytes=20 << 20),
        cost_estimate=pl.CostEstimate(
            flops=2 * width * columns * rows, bytes_accessed=4 * width * columns, transcendentals=0
        ),
    )(acc, before, left, own, other, *acts)
    return act, out, total.reshape(columns)


def pipelined(chips, samples, weight, bias, upstream):
    _, width = samples.shape
    columns = weight.shape[1]
    half = upstream.shape[0]
    core, is_end, owners = places()
    samples, weight, core, other, is_end, owner = lax.optimization_barrier(
        (samples, weight, core, 1 - core, is_end, owners[-1])
    )
    flat_bias, bias = bias, bias.reshape(1, columns)

    def along(value, pairs):
        return lax.ppermute(value, "batch", pairs)

    def across(value, masks):
        return lax.ppermute(value, "sensor", [(i, i ^ masks[i % 2]) for i in range(2 * chips)])

    outer = [(0, 1), (1, 0), (2, 3), (3, 2)]
    inner = [(1, 2), (2, 1)]
    outward = [(1, 0), (2, 3)]
    step = width // HALVES

    def halves(value):
        parts = []
        for h in range(HALVES):
            parts.append(loaded(value, h * step, step))
        return parts

    held = loaded(weight, 0, columns)
    first = along(samples, outer)
    middle = [along(v, inner) for v in halves(samples)]
    far = [along(v, inner) for v in halves(first)]
    middle_out = [along(v, outward) for v in middle]
    far_out = [along(v, outward) for v in far]
    slots = [
        [samples],
        [first],
        [jnp.where(is_end, a, b) for a, b in zip(middle_out, middle)],
        [jnp.where(is_end, a, b) for a, b in zip(far_out, far)],
    ]
    lefts = []
    for parts in slots:
        lefts.append(transposed(parts))

    def picked(array, index, axis=0):
        size = [1 if d == axis else n for d, n in enumerate(array.shape)]
        start = [index if d == axis else 0 for d in range(array.ndim)]
        return lax.dynamic_slice(array, start, size, allow_negative_indices=False).squeeze(axis)

    ups = jnp.stack([upstream] + [across(upstream, (2 * m, 2 * m)) for m in range(1, chips)])

    def product(j):
        total, at = None, 0
        for part in slots[j]:
            term = jnp.dot(part, held[at : at + part.shape[1]], preferred_element_type=jnp.float32)
            total = lax.optimization_barrier(term) if total is None else total + term
            at += part.shape[1]
        return total

    def chip_sum(members):
        value = jnp.stack([product(j) for j in members]).reshape(len(members), 2, half, columns)
        return picked(value, core, 1) + across(picked(value, other, 1), (1, 1))

    def finished(own, got, members):
        grad, act = outcome(members, own, got, bias, ups)
        return grad, across(grad, (1, 1)), act

    x_then_y, y_then_x = (2, 4), (4, 2)
    early = chip_sum([0, 1])
    early = early + across(early, x_then_y)
    both = jnp.concatenate([early, chip_sum([2])])
    got = across(both, y_then_x)
    third = both[2:] + got[2:]
    third_got = across(third, x_then_y)
    last = chip_sum([3])
    last = last + across(last, x_then_y)
    last_got = across(last, y_then_x)
    value = jnp.tanh(last + last_got + flat_bias)
    grad = (picked(ups, owner)[None].astype(jnp.float32) * (1.0 - value * value)).astype(jnp.bfloat16)
    act = value.astype(jnp.bfloat16)
    mine, theirs, acts = zip(
        finished(early, got[:2], (0, 1)), finished(third, third_got, (2,)), (grad, across(grad, (1, 1)), act)
    )
    acc, before = early_gradient(lefts[:-1], mine[:-1], theirs[:-1])
    return finish(acc, before, lefts[-1], mine[-1], theirs[-1], acts)


def solution(mesh):
    placed = (P("batch", "sensor"), P("sensor", "batch"), P("batch"), P("sensor", "batch"))
    sensors, batch = mesh.shape["sensor"], mesh.shape["batch"]

    def body(samples, weight, bias, upstream):
        return pipelined(sensors // 2, samples, weight, bias, upstream)

    fits = batch == 4 and sensors == 2 * batch
    return jax.shard_map(
        body if fits else plain,
        mesh=mesh,
        in_specs=placed,
        out_specs=(P("sensor", "batch"), P("sensor", "batch"), P("batch")),
        check_vma=False,
    )
```

```python
import functools

import jax
import jax.numpy as jnp
from jax import lax
from jax.experimental import pallas as pl
from jax.experimental.pallas import tpu as pltpu
from jax.sharding import PartitionSpec as P


HALVES = 2
TILES = 8
VMEM = pl.BlockSpec(memory_space=pltpu.VMEM)


def plain(samples, branch_weight, branch_bias, upstream):
    all_rows = lax.all_gather(samples, "batch", axis=0, tiled=True)
    partial_value = jnp.dot(all_rows, branch_weight, preferred_element_type=jnp.float32)
    summed = lax.psum_scatter(partial_value, "sensor", scatter_dimension=0, tiled=True)
    pre = summed + branch_bias[None, :]
    act_full = jnp.tanh(pre)
    activation = act_full.astype(jnp.bfloat16)
    grad_pre = (upstream.astype(jnp.float32) * (1.0 - act_full * act_full)).astype(jnp.bfloat16)
    grad_all = lax.all_gather(grad_pre, "sensor", axis=0, tiled=True)
    weight_full = lax.dot_general(
        all_rows, grad_all, (((0,), (0,)), ((), ())), preferred_element_type=jnp.float32
    )
    row_total = jnp.sum(grad_all.astype(jnp.float32), axis=0)
    return activation, weight_full.astype(jnp.bfloat16), row_total


def transpose_kernel(*refs):
    ins, out = refs[:-1], refs[-1]
    at = 0
    for ref in ins:
        width = ref.shape[1]
        out[at : at + width, :] = ref[...].T
        at += width


def stack_kernel(top, bottom, out):
    tile = out.shape[1]
    for at in range(0, out.shape[0], tile):
        both = jnp.concatenate([top[:, at : at + tile], bottom[:, at : at + tile]], axis=0)
        out[at : at + tile, :] = both.T


def transposed(parts, stacked=False):
    rows = parts[0].shape[0] * (len(parts) if stacked else 1)
    width = parts[0].shape[1] if stacked else sum(p.shape[1] for p in parts)
    nbytes = rows * width * 2
    return pl.pallas_call(
        stack_kernel if stacked else transpose_kernel,
        out_shape=jax.ShapeDtypeStruct((width, rows), parts[0].dtype),
        in_specs=[VMEM] * len(parts),
        out_specs=VMEM,
        compiler_params=pltpu.CompilerParams(vmem_limit_bytes=8 << 20),
        cost_estimate=pl.CostEstimate(flops=nbytes * 64, bytes_accessed=2 * nbytes, transcendentals=0),
    )(*parts)


def load_kernel(start, source, out, sem):
    copy = pltpu.make_async_copy(source.at[:, start : start + out.shape[1]], out, sem)
    copy.start()
    copy.wait()


def loaded(samples, start, width):
    rows = samples.shape[0]
    return pl.pallas_call(
        functools.partial(load_kernel, start),
        out_shape=jax.ShapeDtypeStruct((rows, width), samples.dtype),
        in_specs=[pl.BlockSpec(memory_space=pltpu.HBM)],
        out_specs=VMEM,
        scratch_shapes=[pltpu.SemaphoreType.DMA],
        compiler_params=pltpu.CompilerParams(vmem_limit_bytes=4 << 20),
        cost_estimate=pl.CostEstimate(flops=1 << 20, bytes_accessed=4 * rows * width, transcendentals=0),
    )(samples)


def places():
    z, s = lax.axis_index("batch"), lax.axis_index("sensor")
    core, chip = s & 1, s >> 1
    is_end = (z == 0) | (z == 3)
    blocks = [z, z ^ 1, z ^ jnp.where(is_end, 2, 3), z ^ jnp.where(is_end, 3, 2)]
    return core, is_end, [b ^ chip for b in blocks]


def cut_kernel(own, source, out, sem):
    core = places()[0]
    height = out.shape[0]
    start = pl.multiple_of((core if own else 1 - core) * height, height)
    copy = pltpu.make_async_copy(source.at[pl.ds(start, height), :], out, sem)
    copy.start()
    copy.wait()


def cut(block, own):
    rows, width = block.shape
    return pl.pallas_call(
        functools.partial(cut_kernel, own),
        out_shape=jax.ShapeDtypeStruct((rows // 2, width), block.dtype),
        in_specs=[VMEM],
        out_specs=VMEM,
        scratch_shapes=[pltpu.SemaphoreType.DMA],
        compiler_params=pltpu.CompilerParams(vmem_limit_bytes=4 << 20),
        cost_estimate=pl.CostEstimate(flops=1 << 20, bytes_accessed=2 * rows * width, transcendentals=0),
    )(block)


def outcome_kernel(members, own, got, bias, ups, grad, act):
    _, _, owners = places()
    for i, member in enumerate(members):
        value = jnp.tanh(own[i] + got[i] + bias[...])
        act[i] = value.astype(act.dtype)
        grad[i] = (ups[owners[member]].astype(jnp.float32) * (1.0 - value * value)).astype(grad.dtype)


def outcome(members, own, got, bias, ups):
    shape = jax.ShapeDtypeStruct(own.shape, ups.dtype)
    return pl.pallas_call(
        functools.partial(outcome_kernel, members),
        out_shape=(shape, shape),
        in_specs=[VMEM] * 4,
        out_specs=(VMEM, VMEM),
        compiler_params=pltpu.CompilerParams(vmem_limit_bytes=4 << 20),
        cost_estimate=pl.CostEstimate(flops=own.size * 8, bytes_accessed=own.size * 12, transcendentals=own.size),
    )(own, got, bias, ups)


def gather_rows(grad, core, mine, theirs):
    slot = 0
    for own, other in zip(mine, theirs):
        count, half, _ = own.shape
        for i in range(count):
            base = slot * 2 * half
            grad[pl.ds(pl.multiple_of(base + core * half, half), half), :] = own[i]
            grad[pl.ds(pl.multiple_of(base + (1 - core) * half, half), half), :] = other[i]
            slot += 1


def tiles(width):
    tile = width // TILES
    return [slice(k * tile, (k + 1) * tile) for k in range(TILES)]


def early_kernel(slots, rounds, *refs):
    lefts, refs = refs[:slots], refs[slots:]
    mine, theirs, refs = refs[:rounds], refs[rounds : 2 * rounds], refs[2 * rounds :]
    acc, total, grad = refs
    gather_rows(grad, places()[0], mine, theirs)
    for rows in tiles(acc.shape[0]):
        left = jnp.concatenate([ref[rows, :] for ref in lefts], axis=1)
        acc[rows, :] = jnp.dot(left, grad[...], preferred_element_type=jnp.float32)
    total[...] = jnp.sum(grad[...].astype(jnp.float32), axis=0, keepdims=True)


def finish_kernel(counts, acc, before, left, own, other, *refs):
    acts, refs = refs[: len(counts)], refs[len(counts) :]
    out, act_out, total_out, grad, staged, act_staged, total, sems = refs
    _, _, owners = places()
    slot = 0
    for count, act in zip(counts, acts):
        for i in range(count):

            @pl.when(owners[slot] == 0)
            def _(act=act, i=i):
                act_staged[...] = act[i]

            slot += 1
    sends = [pltpu.make_async_copy(act_staged, act_out, sems.at[0])]
    sends[0].start()
    half = own.shape[1]
    grad[:half, :] = own[0]
    grad[half:, :] = other[0]
    for k, rows in enumerate(tiles(acc.shape[0])):
        term = jnp.dot(left[rows, :], grad[...], preferred_element_type=jnp.float32)
        staged[rows, :] = (acc[rows, :] + term).astype(staged.dtype)
        send = pltpu.make_async_copy(staged.at[rows, :], out.at[rows, :], sems.at[2 + k])
        send.start()
        sends.append(send)
    pair = own[0].astype(jnp.float32) + other[0].astype(jnp.float32)
    total[...] = before[...] + jnp.sum(pair, axis=0, keepdims=True)
    send = pltpu.make_async_copy(total, total_out, sems.at[1])
    send.start()
    sends.append(send)
    for send in sends:
        send.wait()


def early_gradient(lefts, mine, theirs):
    width, rows = lefts[0].shape
    columns = mine[0].shape[2]
    depth = rows * len(lefts)
    return pl.pallas_call(
        functools.partial(early_kernel, len(lefts), len(mine)),
        out_shape=(
            jax.ShapeDtypeStruct((width, columns), jnp.float32),
            jax.ShapeDtypeStruct((1, columns), jnp.float32),
        ),
        in_specs=[VMEM] * (len(lefts) + 2 * len(mine)),
        out_specs=(VMEM, VMEM),
        scratch_shapes=[pltpu.VMEM((depth, columns), mine[0].dtype)],
        compiler_params=pltpu.CompilerParams(vmem_limit_bytes=16 << 20),
        cost_estimate=pl.CostEstimate(
            flops=2 * width * columns * depth, bytes_accessed=4 * width * columns, transcendentals=0
        ),
    )(*lefts, *mine, *theirs)


def finish(acc, before, left, own, other, acts):
    width, rows = left.shape
    counts = tuple(a.shape[0] for a in acts)
    _, half, columns = own.shape
    hbm = pl.BlockSpec(memory_space=pl.ANY)
    kind = own.dtype
    out, act, total = pl.pallas_call(
        functools.partial(finish_kernel, counts),
        out_shape=(
            jax.ShapeDtypeStruct((width, columns), kind),
            jax.ShapeDtypeStruct((half, columns), kind),
            jax.ShapeDtypeStruct((1, columns), jnp.float32),
        ),
        in_specs=[VMEM] * (5 + len(acts)),
        out_specs=(hbm, hbm, hbm),
        scratch_shapes=[
            pltpu.VMEM((rows, columns), kind),
            pltpu.VMEM((width, columns), kind),
            pltpu.VMEM((half, columns), kind),
            pltpu.VMEM((1, columns), jnp.float32),
            pltpu.SemaphoreType.DMA((2 + TILES,)),
        ],
        compiler_params=pltpu.CompilerParams(vmem_limit_bytes=20 << 20),
        cost_estimate=pl.CostEstimate(
            flops=2 * width * columns * rows, bytes_accessed=4 * width * columns, transcendentals=0
        ),
    )(acc, before, left, own, other, *acts)
    return act, out, total.reshape(columns)


def pipelined(chips, samples, weight, bias, upstream):
    _, width = samples.shape
    columns = weight.shape[1]
    half = upstream.shape[0]
    core, is_end, owners = places()
    samples, weight, core, other, is_end, owner = lax.optimization_barrier(
        (samples, weight, core, 1 - core, is_end, owners[-1])
    )
    flat_bias, bias = bias, bias.reshape(1, columns)

    def along(value, pairs):
        return lax.ppermute(value, "batch", pairs)

    def across(value, masks):
        return lax.ppermute(value, "sensor", [(i, i ^ masks[i % 2]) for i in range(2 * chips)])

    def crossed(value, pairs):
        both = [(i * chips + a, (i ^ 1) * chips + b) for i in range(2 * chips) for a, b in pairs]
        return lax.ppermute(value, ("sensor", "batch"), both)

    outer = [(0, 1), (1, 0), (2, 3), (3, 2)]
    inner = [(1, 2), (2, 1)]
    outward = [(1, 0), (2, 3)]
    step = width // HALVES

    def halves(value):
        parts = []
        for h in range(HALVES):
            parts.append(loaded(value, h * step, step))
        return parts

    held = loaded(weight, 0, columns)
    first = along(samples, outer)
    middle = [along(v, inner) for v in halves(samples)]
    held_other = across(held, (1, 1))
    own_rows = cut(first, True)
    other_rows = cut(first, False)
    far = [along(own_rows, inner), crossed(other_rows, inner)]
    middle_out = [along(v, outward) for v in middle]
    far_out = [along(v, outward) for v in far]
    slots = [
        [samples],
        [first],
        [jnp.where(is_end, a, b) for a, b in zip(middle_out, middle)],
        [jnp.where(is_end, a, b) for a, b in zip(far_out, far)],
    ]
    lefts = []
    for parts in slots[:3]:
        lefts.append(transposed(parts))
    last_rows = across(slots[3][1], (1, 1))
    lefts.append(transposed([slots[3][0], last_rows], stacked=True))

    def picked(array, index, axis=0):
        size = [1 if d == axis else n for d, n in enumerate(array.shape)]
        start = [index if d == axis else 0 for d in range(array.ndim)]
        return lax.dynamic_slice(array, start, size, allow_negative_indices=False).squeeze(axis)

    ups = jnp.stack([upstream] + [across(upstream, (2 * m, 2 * m)) for m in range(1, chips)])

    def product(j, weights):
        total, at = None, 0
        for h, part in enumerate(slots[j]):
            rows = weights[h] if j == 3 else weights[at : at + part.shape[1]]
            term = jnp.dot(part, rows, preferred_element_type=jnp.float32)
            total = lax.optimization_barrier(term) if total is None else total + term
            at += part.shape[1]
        return total

    def chip_sum(members):
        value = jnp.stack([product(j, held) for j in members]).reshape(len(members), 2, half, columns)
        return picked(value, core, 1) + across(picked(value, other, 1), (1, 1))

    def finished(own, got, members):
        grad, act = outcome(members, own, got, bias, ups)
        return grad, across(grad, (1, 1)), act

    x_then_y, y_then_x = (2, 4), (4, 2)
    early = chip_sum([0, 1])
    early = early + across(early, x_then_y)
    both = jnp.concatenate([early, chip_sum([2])])
    got = across(both, y_then_x)
    third = both[2:] + got[2:]
    third_got = across(third, x_then_y)
    last = product(3, [held, held_other])[None]
    last = last + across(last, x_then_y)
    last_got = across(last, y_then_x)
    value = jnp.tanh(last + last_got + flat_bias)
    grad = (picked(ups, owner)[None].astype(jnp.float32) * (1.0 - value * value)).astype(jnp.bfloat16)
    act = value.astype(jnp.bfloat16)
    mine, theirs, acts = zip(
        finished(early, got[:2], (0, 1)), finished(third, third_got, (2,)), (grad, across(grad, (1, 1)), act)
    )
    acc, before = early_gradient(lefts[:-1], mine[:-1], theirs[:-1])
    return finish(acc, before, lefts[-1], mine[-1], theirs[-1], acts)


def solution(mesh):
    placed = (P("batch", "sensor"), P("sensor", "batch"), P("batch"), P("sensor", "batch"))
    sensors, batch = mesh.shape["sensor"], mesh.shape["batch"]

    def body(samples, weight, bias, upstream):
        return pipelined(sensors // 2, samples, weight, bias, upstream)

    fits = batch == 4 and sensors == 2 * batch
    return jax.shard_map(
        body if fits else plain,
        mesh=mesh,
        in_specs=placed,
        out_specs=(P("sensor", "batch"), P("sensor", "batch"), P("batch")),
        check_vma=False,
    )
```

```python
import functools

import jax
import jax.numpy as jnp
from jax import lax
from jax.experimental import pallas as pl
from jax.experimental.pallas import tpu as pltpu
from jax.sharding import PartitionSpec as P


HALVES = 2
TILES = 8
VMEM = pl.BlockSpec(memory_space=pltpu.VMEM)


def plain(samples, branch_weight, branch_bias, upstream):
    all_rows = lax.all_gather(samples, "batch", axis=0, tiled=True)
    partial_value = jnp.dot(all_rows, branch_weight, preferred_element_type=jnp.float32)
    summed = lax.psum_scatter(partial_value, "sensor", scatter_dimension=0, tiled=True)
    pre = summed + branch_bias[None, :]
    act_full = jnp.tanh(pre)
    activation = act_full.astype(jnp.bfloat16)
    grad_pre = (upstream.astype(jnp.float32) * (1.0 - act_full * act_full)).astype(jnp.bfloat16)
    grad_all = lax.all_gather(grad_pre, "sensor", axis=0, tiled=True)
    weight_full = lax.dot_general(
        all_rows, grad_all, (((0,), (0,)), ((), ())), preferred_element_type=jnp.float32
    )
    row_total = jnp.sum(grad_all.astype(jnp.float32), axis=0)
    return activation, weight_full.astype(jnp.bfloat16), row_total


def transpose_kernel(*refs):
    ins, out = refs[:-1], refs[-1]
    at = 0
    for ref in ins:
        width = ref.shape[1]
        out[at : at + width, :] = ref[...].T
        at += width


def stack_kernel(top, bottom, out):
    tile = out.shape[1]
    for at in range(0, out.shape[0], tile):
        both = jnp.concatenate([top[:, at : at + tile], bottom[:, at : at + tile]], axis=0)
        out[at : at + tile, :] = both.T


def transposed(parts, stacked=False):
    rows = parts[0].shape[0] * (len(parts) if stacked else 1)
    width = parts[0].shape[1] if stacked else sum(p.shape[1] for p in parts)
    nbytes = rows * width * 2
    return pl.pallas_call(
        stack_kernel if stacked else transpose_kernel,
        out_shape=jax.ShapeDtypeStruct((width, rows), parts[0].dtype),
        in_specs=[VMEM] * len(parts),
        out_specs=VMEM,
        compiler_params=pltpu.CompilerParams(vmem_limit_bytes=8 << 20),
        cost_estimate=pl.CostEstimate(flops=nbytes * 64, bytes_accessed=2 * nbytes, transcendentals=0),
    )(*parts)


def load_kernel(start, source, out, sem):
    copy = pltpu.make_async_copy(source.at[:, start : start + out.shape[1]], out, sem)
    copy.start()
    copy.wait()


def loaded(samples, start, width):
    rows = samples.shape[0]
    return pl.pallas_call(
        functools.partial(load_kernel, start),
        out_shape=jax.ShapeDtypeStruct((rows, width), samples.dtype),
        in_specs=[pl.BlockSpec(memory_space=pltpu.HBM)],
        out_specs=VMEM,
        scratch_shapes=[pltpu.SemaphoreType.DMA],
        compiler_params=pltpu.CompilerParams(vmem_limit_bytes=4 << 20),
        cost_estimate=pl.CostEstimate(flops=1 << 20, bytes_accessed=4 * rows * width, transcendentals=0),
    )(samples)


def parity(value):
    return (value ^ (value >> 1) ^ (value >> 2)) & 1


def places():
    z, s = lax.axis_index("batch"), lax.axis_index("sensor")
    core, chip = s & 1, s >> 1
    is_end = (z == 0) | (z == 3)
    blocks = [z, z ^ 1, z ^ jnp.where(is_end, 2, 3), z ^ jnp.where(is_end, 3, 2)]
    owners = [b ^ chip for b in blocks]
    return [core ^ parity(owner) for owner in owners], is_end, owners


def cut_kernel(own, source, out, sem):
    kept = places()[0][1]
    height = out.shape[0]
    start = pl.multiple_of((kept if own else 1 - kept) * height, height)
    copy = pltpu.make_async_copy(source.at[pl.ds(start, height), :], out, sem)
    copy.start()
    copy.wait()


def cut(block, own):
    rows, width = block.shape
    return pl.pallas_call(
        functools.partial(cut_kernel, own),
        out_shape=jax.ShapeDtypeStruct((rows // 2, width), block.dtype),
        in_specs=[VMEM],
        out_specs=VMEM,
        scratch_shapes=[pltpu.SemaphoreType.DMA],
        compiler_params=pltpu.CompilerParams(vmem_limit_bytes=4 << 20),
        cost_estimate=pl.CostEstimate(flops=1 << 20, bytes_accessed=2 * rows * width, transcendentals=0),
    )(block)


def outcome_kernel(members, own, got, bias, ups, grad, act):
    _, _, owners = places()
    for i, member in enumerate(members):
        value = jnp.tanh(own[i] + got[i] + bias[...])
        act[i] = value.astype(act.dtype)
        grad[i] = (ups[owners[member]].astype(jnp.float32) * (1.0 - value * value)).astype(grad.dtype)


def outcome(members, own, got, bias, ups):
    shape = jax.ShapeDtypeStruct(own.shape, ups.dtype)
    return pl.pallas_call(
        functools.partial(outcome_kernel, members),
        out_shape=(shape, shape),
        in_specs=[VMEM] * 4,
        out_specs=(VMEM, VMEM),
        compiler_params=pltpu.CompilerParams(vmem_limit_bytes=4 << 20),
        cost_estimate=pl.CostEstimate(flops=own.size * 8, bytes_accessed=own.size * 12, transcendentals=own.size),
    )(own, got, bias, ups)


def gather_rows(grad, kept, mine, theirs):
    slot = 0
    for own, other in zip(mine, theirs):
        count, half, _ = own.shape
        for i in range(count):
            base = slot * 2 * half
            grad[pl.ds(pl.multiple_of(base + kept[slot] * half, half), half), :] = own[i]
            grad[pl.ds(pl.multiple_of(base + (1 - kept[slot]) * half, half), half), :] = other[i]
            slot += 1


def tiles(width):
    tile = width // TILES
    return [slice(k * tile, (k + 1) * tile) for k in range(TILES)]


def early_kernel(slots, rounds, *refs):
    lefts, refs = refs[:slots], refs[slots:]
    mine, theirs, refs = refs[:rounds], refs[rounds : 2 * rounds], refs[2 * rounds :]
    acc, total, grad = refs
    gather_rows(grad, places()[0], mine, theirs)
    for rows in tiles(acc.shape[0]):
        left = jnp.concatenate([ref[rows, :] for ref in lefts], axis=1)
        acc[rows, :] = jnp.dot(left, grad[...], preferred_element_type=jnp.float32)
    total[...] = jnp.sum(grad[...].astype(jnp.float32), axis=0, keepdims=True)


def finish_kernel(counts, acc, before, third, last, third_own, third_other, own, other, *refs):
    acts, refs = refs[: len(counts)], refs[len(counts) :]
    out, act_out, total_out, grad, staged, act_staged, total, sems = refs
    kept, _, owners = places()
    slot = 0
    for count, act in zip(counts, acts):
        for i in range(count):

            @pl.when(owners[slot] == 0)
            def _(act=act, i=i):
                act_staged[...] = act[i]

            slot += 1
    sends = [pltpu.make_async_copy(act_staged, act_out, sems.at[0])]
    sends[0].start()
    half = own.shape[1]
    gather_rows(grad, kept[2:], [third_own], [third_other])
    grad[2 * half : 3 * half, :] = own[0]
    grad[3 * half :, :] = other[0]
    for k, rows in enumerate(tiles(acc.shape[0])):
        left = jnp.concatenate([third[rows, :], last[rows, :]], axis=1)
        term = jnp.dot(left, grad[...], preferred_element_type=jnp.float32)
        staged[rows, :] = (acc[rows, :] + term).astype(staged.dtype)
        send = pltpu.make_async_copy(staged.at[rows, :], out.at[rows, :], sems.at[2 + k])
        send.start()
        sends.append(send)
    pairs = [a[0].astype(jnp.float32) + b[0].astype(jnp.float32) for a, b in ((third_own, third_other), (own, other))]
    total[...] = before[...] + jnp.sum(pairs[0] + pairs[1], axis=0, keepdims=True)
    send = pltpu.make_async_copy(total, total_out, sems.at[1])
    send.start()
    sends.append(send)
    for send in sends:
        send.wait()


def early_gradient(lefts, mine, theirs):
    width, rows = lefts[0].shape
    columns = mine[0].shape[2]
    depth = rows * len(lefts)
    return pl.pallas_call(
        functools.partial(early_kernel, len(lefts), len(mine)),
        out_shape=(
            jax.ShapeDtypeStruct((width, columns), jnp.float32),
            jax.ShapeDtypeStruct((1, columns), jnp.float32),
        ),
        in_specs=[VMEM] * (len(lefts) + 2 * len(mine)),
        out_specs=(VMEM, VMEM),
        scratch_shapes=[pltpu.VMEM((depth, columns), mine[0].dtype)],
        compiler_params=pltpu.CompilerParams(vmem_limit_bytes=16 << 20),
        cost_estimate=pl.CostEstimate(
            flops=2 * width * columns * depth, bytes_accessed=4 * width * columns, transcendentals=0
        ),
    )(*lefts, *mine, *theirs)


def finish(acc, before, lefts, mine, theirs, acts):
    width, rows = acc.shape[0], sum(left.shape[1] for left in lefts)
    counts = tuple(a.shape[0] for a in acts)
    _, half, columns = mine[0].shape
    hbm = pl.BlockSpec(memory_space=pl.ANY)
    kind = mine[0].dtype
    out, act, total = pl.pallas_call(
        functools.partial(finish_kernel, counts),
        out_shape=(
            jax.ShapeDtypeStruct((width, columns), kind),
            jax.ShapeDtypeStruct((half, columns), kind),
            jax.ShapeDtypeStruct((1, columns), jnp.float32),
        ),
        in_specs=[VMEM] * (8 + len(acts)),
        out_specs=(hbm, hbm, hbm),
        scratch_shapes=[
            pltpu.VMEM((rows, columns), kind),
            pltpu.VMEM((width, columns), kind),
            pltpu.VMEM((half, columns), kind),
            pltpu.VMEM((1, columns), jnp.float32),
            pltpu.SemaphoreType.DMA((2 + TILES,)),
        ],
        compiler_params=pltpu.CompilerParams(vmem_limit_bytes=20 << 20),
        cost_estimate=pl.CostEstimate(
            flops=2 * width * columns * rows, bytes_accessed=4 * width * columns, transcendentals=0
        ),
    )(acc, before, *lefts, mine[0], theirs[0], mine[1], theirs[1], *acts)
    return act, out, total.reshape(columns)


def pipelined(chips, samples, weight, bias, upstream):
    _, width = samples.shape
    columns = weight.shape[1]
    half = upstream.shape[0]
    kept, is_end, owners = places()
    samples, weight, kept, given, is_end, owner = lax.optimization_barrier(
        (samples, weight, kept[:3], [1 - k for k in kept[:3]], is_end, owners[-1])
    )
    flat_bias, bias = bias, bias.reshape(1, columns)

    def along(value, pairs):
        return lax.ppermute(value, "batch", pairs)

    def across(value, masks):
        return lax.ppermute(value, "sensor", [(i, i ^ masks[parity(i)]) for i in range(2 * chips)])

    def crossed(value, pairs):
        both = [(i * chips + a, (i ^ 1) * chips + b) for i in range(2 * chips) for a, b in pairs]
        return lax.ppermute(value, ("sensor", "batch"), both)

    outer = [(0, 1), (1, 0), (2, 3), (3, 2)]
    inner = [(1, 2), (2, 1)]
    outward = [(1, 0), (2, 3)]
    step = width // HALVES

    def halves(value):
        parts = []
        for h in range(HALVES):
            parts.append(loaded(value, h * step, step))
        return parts

    held = loaded(weight, 0, columns)
    first = along(samples, outer)
    middle = [along(v, inner) for v in halves(samples)]
    held_other = across(held, (1, 1))
    own_rows = cut(first, True)
    other_rows = cut(first, False)
    far = [along(own_rows, inner), crossed(other_rows, inner)]
    middle_out = [along(v, outward) for v in middle]
    far_out = [along(v, outward) for v in far]
    slots = [
        [samples],
        [first],
        [jnp.where(is_end, a, b) for a, b in zip(middle_out, middle)],
        [jnp.where(is_end, a, b) for a, b in zip(far_out, far)],
    ]
    lefts = []
    for parts in slots[:3]:
        lefts.append(transposed(parts))
    last_rows = across(slots[3][1], (1, 1))
    lefts.append(transposed([slots[3][0], last_rows], stacked=True))

    def picked(array, index, axis=0):
        size = [1 if d == axis else n for d, n in enumerate(array.shape)]
        start = [index if d == axis else 0 for d in range(array.ndim)]
        return lax.dynamic_slice(array, start, size, allow_negative_indices=False).squeeze(axis)

    ups = jnp.stack([upstream] + [across(upstream, (2 * m + parity(m),) * 2) for m in range(1, chips)])

    def product(j, weights):
        total, at = None, 0
        for h, part in enumerate(slots[j]):
            rows = weights[h] if j == 3 else weights[at : at + part.shape[1]]
            term = jnp.dot(part, rows, preferred_element_type=jnp.float32)
            total = lax.optimization_barrier(term) if total is None else total + term
            at += part.shape[1]
        return total

    def chip_sum(members):
        parts = [product(j, held).reshape(2, half, columns) for j in members]
        own = jnp.stack([picked(part, kept[j]) for j, part in zip(members, parts)])
        sent = jnp.stack([picked(part, given[j]) for j, part in zip(members, parts)])
        return own + across(sent, (1, 1))

    def finished(own, got, members):
        grad, act = outcome(members, own, got, bias, ups)
        return grad, across(grad, (1, 1)), act

    x_then_y, y_then_x = (3, 5), (5, 3)
    early = chip_sum([0, 1])
    early = early + across(early, x_then_y)
    both = jnp.concatenate([early, chip_sum([2])])
    got = across(both, y_then_x)
    third = both[2:] + got[2:]
    third_got = across(third, x_then_y)
    last = product(3, [held, held_other])[None]
    last = last + across(last, x_then_y)
    last_got = across(last, y_then_x)
    value = jnp.tanh(last + last_got + flat_bias)
    grad = (picked(ups, owner)[None].astype(jnp.float32) * (1.0 - value * value)).astype(jnp.bfloat16)
    act = value.astype(jnp.bfloat16)
    mine, theirs, acts = zip(
        finished(early, got[:2], (0, 1)), finished(third, third_got, (2,)), (grad, across(grad, (1, 1)), act)
    )
    acc, before = early_gradient(lefts[:2], mine[:1], theirs[:1])
    return finish(acc, before, lefts[2:], mine[1:], theirs[1:], acts)


def solution(mesh):
    placed = (P("batch", "sensor"), P("sensor", "batch"), P("batch"), P("sensor", "batch"))
    sensors, batch = mesh.shape["sensor"], mesh.shape["batch"]

    def body(samples, weight, bias, upstream):
        return pipelined(sensors // 2, samples, weight, bias, upstream)

    fits = batch == 4 and sensors == 2 * batch
    return jax.shard_map(
        body if fits else plain,
        mesh=mesh,
        in_specs=placed,
        out_specs=(P("sensor", "batch"), P("sensor", "batch"), P("batch")),
        check_vma=False,
    )
```
